512 devices in a mesh: row: 32 (over x, y), col: 16 (over z, core).
Axes of the slice: x: 4, y: 8, z: 8, core: 2. Of those that a mesh axis runs over, the one named last changes fastest.
Arguments:
- activations: bfloat16 [2048, 16384], P('row', 'col'), may hold values from -6 to 6
- cotangents: bfloat16 [2048, 16384], P('col', 'row'), may hold values from -6 to 6
- weights: bfloat16 [16384, 16384], P('row', 'col'), may hold values from -6 to 6
- momentum: bfloat16 [16384, 16384], P('row', 'col'), may hold values from -16 to 16
- right_basis: float32 [64, 16384], P(None, 'col'), may hold values from -1 to 1
- next_inputs: bfloat16 [1024, 16384], P('row', 'col'), may hold values from -6 to 6
Outputs:
- weights_new: bfloat16 [16384, 16384], P('row', 'col')
- momentum_new: bfloat16 [16384, 16384], P('row', 'col')
- basis_new: float32 [64, 16384], P(None, 'col')
- outputs: bfloat16 [1024, 16384], P('col', 'row')
The draws below stay inside these ranges and needn't reach their ends.
All inputs are finite; a program needn't handle non-finite values.
Results may differ from the reference program's by a relative error of at most 0.02.
Values may be sent and summed in bfloat16 or wider, within the bound.
A program may use at most 64 MiB of HBM per device.

```python
import math
import jax
import jax.numpy as jnp
from jax import lax

DOUT = 16384
DIN = 16384
RANK = 64
TOKENS = 2048
NEXT = 1024
N_COL = 16


def drawn_parts(key):
    base = jax.random.fold_in(key, 5171)
    left_key, right_key, scale_key = jax.random.split(base, 3)
    left_vectors = jax.random.normal(left_key, (DOUT, RANK), jnp.float32) / math.sqrt(DOUT)
    right_vectors = jax.random.normal(right_key, (RANK, DIN), jnp.float32) / math.sqrt(DIN)
    strengths = jnp.exp(jax.random.uniform(scale_key, (RANK,), jnp.float32, 0.0, math.log(3.0)))
    return (left_vectors, right_vectors, strengths)


def draw_momentum(key, part):
    left_vectors, right_vectors, strengths = drawn_parts(key)
    bulk_key = jax.random.fold_in(key, 17)
    bulk_part = jax.random.normal(bulk_key, (DOUT, DIN), jnp.float32)
    amplitude = 1.2 * math.sqrt(DOUT * DIN / RANK)
    aligned = jnp.dot(left_vectors * (amplitude * strengths)[None, :], right_vectors, precision=lax.Precision.HIGHEST)
    return jnp.clip(bulk_part + aligned, -16.0, 16.0).astype(jnp.bfloat16)


def draw_right_basis(key, part):
    left_vectors, right_vectors, strengths = drawn_parts(key)
    noise_key = jax.random.fold_in(key, 29)
    noise_part = jax.random.normal(noise_key, (RANK, DIN), jnp.float32)
    return jnp.clip(right_vectors + 0.5 * noise_part / math.sqrt(DIN), -1.0, 1.0)


def level_of(stream_key, shape, cuts, low, largest):
    def one(position, blocks):
        heights = jax.random.uniform(jax.random.fold_in(jax.random.fold_in(stream_key, 6), position), (blocks,), jnp.float32, low / len(cuts), largest / len(cuts))
        return jnp.repeat(jnp.exp(heights), shape[position] // blocks).reshape((-1,) + (1,) * (len(shape) - position - 1))

    loudness = one(*cuts[0])
    for cut in cuts[1:]:
        loudness = loudness * one(*cut)
    return loudness


def centred(rng, dims, spread, most, cuts=(), kind=jnp.bfloat16):
    factor_of = level_of(rng, dims, cuts, -0.22, 0.18) if cuts else 1.0
    array = jax.random.normal(rng, dims, jnp.float32) * spread * factor_of
    return jnp.minimum(jnp.maximum(array, -most), most).astype(kind)


def setup_inputs(seed: int = 0) -> dict:
    key_of = jax.random.split(jax.random.key(seed), 7)
    activations = centred(key_of[0], (TOKENS, DIN), 1.0, 6.0, ((0, 32), (1, 16)))
    cotangents = centred(key_of[1], (TOKENS, DOUT), 1.0, 6.0, ((0, 16), (1, 32)))
    weights = centred(key_of[2], (DOUT, DIN), 1.0, 6.0, ((0, 32), (1, 16)))
    momentum = draw_momentum(jax.random.fold_in(key_of[6], 71), 0)
    right_basis = draw_right_basis(jax.random.fold_in(key_of[6], 71), 0)
    next_inputs = centred(key_of[5], (NEXT, DIN), 1.0, 6.0, ((0, 32), (1, 16)))
    return dict(activations=activations, cotangents=cotangents, weights=weights, momentum=momentum, right_basis=right_basis, next_inputs=next_inputs)


momentum_decay = 0.95
learn_rate = 0.3
norm_eps = 1e-06

def reference(activations, cotangents, weights, momentum, right_basis, next_inputs):
    highest = lax.Precision.HIGHEST
    gradient = jnp.dot(cotangents.T.astype(jnp.float32), activations.astype(jnp.float32), preferred_element_type=jnp.float32) / math.sqrt(TOKENS)
    buffer = momentum.astype(jnp.float32) + gradient
    left_factor = jnp.dot(right_basis, buffer.T, precision=highest)
    gram_matrix = jnp.dot(left_factor, left_factor.T, precision=highest)
    factor = jnp.linalg.cholesky(gram_matrix)
    orth_basis = lax.linalg.triangular_solve(factor, left_factor, left_side=True, lower=True)
    right_factor = jnp.dot(orth_basis, buffer, precision=highest)
    feedback = jnp.dot(orth_basis.T, right_factor, precision=highest)
    momentum_new = (buffer - (1.0 - momentum_decay) * feedback).astype(jnp.bfloat16)
    squares = lax.optimization_barrier(jnp.sum(right_factor * right_factor, axis=1))
    basis_new = right_factor / jnp.sqrt(squares + norm_eps)[:, None]
    update = jnp.dot(orth_basis.T, basis_new, precision=highest)
    step_scale = learn_rate * math.sqrt(DOUT * DIN / RANK)
    weights_new = (weights.astype(jnp.float32) - step_scale * update).astype(jnp.bfloat16)
    block_width = DIN // N_COL

    def add_block(running, block_index):
        start = (block_index * block_width).astype(jnp.int32)
        input_block = lax.dynamic_slice_in_dim(next_inputs, start, block_width, 1)
        weight_block = lax.dynamic_slice_in_dim(weights_new, start, block_width, 1)
        partial_value = jnp.dot(input_block.astype(jnp.float32), weight_block.T.astype(jnp.float32), preferred_element_type=jnp.float32) / math.sqrt(DIN)
        rounded = lax.optimization_barrier(partial_value.astype(jnp.bfloat16))
        return (running + rounded.astype(running.dtype), None)
    summed, _ = lax.scan(add_block, jnp.zeros((NEXT, DOUT), jnp.float32), jnp.arange(N_COL, dtype=jnp.int32))
    outputs = summed.astype(jnp.bfloat16)
    return (weights_new, momentum_new, basis_new, outputs)
```

```python
import heapq
import math

import jax
import jax.numpy as jnp
from jax import lax
from jax.experimental import pallas as pl
from jax.experimental.pallas import tpu as pltpu
from jax.sharding import Mesh
from jax.sharding import PartitionSpec as P

RANK = 64
MESH = pl.DeviceIdType.MESH
momentum_decay = 0.95
learn_rate = 0.3
norm_eps = 1e-06
F32 = jnp.float32
BF16 = jnp.bfloat16
HIGHEST = lax.Precision.HIGHEST

LATENCY = 2.0
RATE = 46e3
START_NEXT = 17.0


def ring_paths(n, tie):
    reach = [d for d in range(1, (n + 1) // 2)]
    out = [d for d in reach] + [-d for d in reach]
    if n % 2 == 0:
        out.append(tie * (n // 2))
    return out


def sign(v):
    return (v > 0) - (v < 0)


def plane_tree(first, sizes):
    n1, n2 = sizes[first], sizes[1 - first]
    tree = {}

    def add(parent, child):
        tree.setdefault(parent, []).append(child)
        tree.setdefault(child, [])

    def place(d1, d2):
        return (d1, d2) if first == 0 else (d2, d1)

    tie = 1 if first == 0 else -1
    stem = sorted([0] + ring_paths(n1, tie), key=abs)
    for d1 in stem:
        if d1:
            add(place(d1 - sign(d1), 0), place(d1, 0))
    for d1 in stem:
        for d2 in sorted(ring_paths(n2, 1 if d1 % 2 else -1), key=abs):
            add(place(d1, d2 - sign(d2)), place(d1, d2))
    return tree


def planned(streams):
    free = {}
    queue = []
    order = []
    for number, stream in enumerate(streams):
        heapq.heappush(queue, (stream["start"], 0, number, stream["root"]))
    while queue:
        now, kind, number, spot = heapq.heappop(queue)
        stream = streams[number]
        order.append((now, number, spot))
        for child in stream["tree"][spot]:
            link = stream["link"](spot, child)
            rate = RATE if link != "pair" else 5e5
            begin = max(now, free.get(link, 0.0))
            free[link] = begin + stream["bytes"] / rate
            heapq.heappush(queue, (free[link] + LATENCY, 1, number, child))
    return order


def split2(v):
    hi = v.astype(BF16)
    return hi, (v - hi.astype(F32)).astype(BF16)


def split3(v):
    hi = v.astype(BF16)
    rest = v - hi.astype(F32)
    mid = rest.astype(BF16)
    return hi, mid, (rest - mid.astype(F32)).astype(BF16)


def dot_nn(a, b, precision=None):
    return lax.dot_general(a, b, (((1,), (0,)), ((), ())), preferred_element_type=F32, precision=precision)


def dot_nt(a, b, precision=None):
    return lax.dot_general(a, b, (((1,), (1,)), ((), ())), preferred_element_type=F32, precision=precision)


def dot_tn(a, b, precision=None):
    return lax.dot_general(a, b, (((0,), (0,)), ((), ())), preferred_element_type=F32, precision=precision)


def build(mesh, shapes):
    nx, ny, nz, nc = (mesh.shape[a] for a in ("x", "y", "z", "c"))
    plane, cols = nx * ny, nz * nc
    t_act, width = shapes["act"]
    t_cot, rows = shapes["cot"]
    n_next = shapes["nxt"][0]
    tokens = t_act * plane
    n_out = n_next * plane // cols
    half = n_out // 2
    d_out, d_in = rows * plane, width * cols
    grad_scale = 1.0 / math.sqrt(tokens)
    out_scale = 1.0 / math.sqrt(d_in)
    step_scale = learn_rate * math.sqrt(d_out * d_in / RANK)
    feed_scale = 1.0 - momentum_decay
    wy = width * 5 // 8
    wx = width - wy
    rpc = RANK // cols
    r_groups = RANK // 16
    c_groups = plane // r_groups
    c_width = width // c_groups

    tree_y, tree_x = plane_tree(1, (nx, ny)), plane_tree(0, (nx, ny))

    def plane_link(a, b):
        return ("x", b[0] - a[0]) if a[1] == b[1] else ("y", b[1] - a[1])

    def cot_tree():
        tree = {}
        for d in sorted([0] + ring_paths(nz, 1), key=abs):
            if d:
                tree[(d - sign(d), 0)].append((d, 0))
            tree[(d, 0)] = [(d, 1)] if nc > 1 else []
            if nc > 1:
                tree[(d, 1)] = []
        return tree

    def cot_link(a, b):
        return "pair" if a[1] != b[1] else ("z", b[0] - a[0])

    streams = [
        dict(tree=tree_y, bytes=t_act * wy * 2, start=0.0, root=(0, 0), link=plane_link, kind="plane"),
        dict(tree=tree_x, bytes=t_act * wx * 2, start=0.0, root=(0, 0), link=plane_link, kind="plane"),
        dict(tree=cot_tree(), bytes=t_cot * rows * 2, start=0.0, root=(0, 0), link=cot_link, kind="col"),
        dict(tree=tree_y, bytes=n_next * wy * 2, start=START_NEXT, root=(0, 0), link=plane_link, kind="plane"),
        dict(tree=tree_x, bytes=n_next * wx * 2, start=START_NEXT, root=(0, 0), link=plane_link, kind="plane"),
    ]
    order = planned(streams)
    ids = {}
    for _, number, spot in order:
        if spot != (0, 0):
            ids[(number, spot)] = len(ids)
    n_bulk = len(ids)

    def kernel(
        act, cot, w_in, m_in, rb, nxt,
        w_out, m_out, b_out, o_out,
        a_y, a_x, c_all, n_y, n_x, c_t, w, m, v,
        buf, b_hi, b_lo,
        u_s, u_r, v_s, v_r, u_m, u_g, u_full, l_s, l_g, left, g_s, g_r, g_m, g_g, gram,
        orth, r_s, r_r, r_m, r_g, rmat,
        p_s, p_r, q_s, q_r, y_s, y_r, s_s, s_r,
        bulk_send, bulk_recv, small_send, small_recv, local_sem,
    ):
        x, y, z, c = (lax.axis_index(a) for a in ("x", "y", "z", "c"))
        me_row, me_col = x * ny + y, z * nc + c
        stores = [a_y, a_x, c_all, n_y, n_x]

        def local(src, dst, k):
            return pltpu.make_async_copy(src, dst, local_sem.at[k])

        ky, kx = pl.ds(0, wy), pl.ds(wy, wx)
        loads = [
            local(act.at[:, ky], a_y.at[me_row], 0),
            local(act.at[:, kx], a_x.at[me_row], 1),
            local(cot, c_all.at[me_col], 2),
            local(rb, v, 3),
            local(m_in, m, 4),
            local(nxt.at[:, ky], n_y.at[me_row], 5),
            local(nxt.at[:, kx], n_x.at[me_row], 6),
            local(w_in, w, 7),
        ]
        for copy in loads:
            copy.start()

        def plane_peer(k):
            return (x + k // ny) % nx, (y + k % ny) % ny

        def col_peer(k):
            return (z + k // nc) % nz, (c + k % nc) % nc

        barrier = pltpu.get_barrier_semaphore()

        def greet_plane(k, carry):
            px, py = plane_peer(k)
            pl.semaphore_signal(barrier, inc=1, device_id={"x": px, "y": py}, device_id_type=MESH)
            return carry

        def greet_col(k, carry):
            pz, pc = col_peer(k)
            pl.semaphore_signal(barrier, inc=1, device_id={"z": pz, "c": pc}, device_id_type=MESH)
            return carry

        lax.fori_loop(1, plane, greet_plane, 0)
        lax.fori_loop(1, cols, greet_col, 0)
        pl.semaphore_wait(barrier, plane - 1 + cols - 1)

        def origin_slot(number, spot):
            if streams[number]["kind"] == "plane":
                return ((x - spot[0]) % nx) * ny + (y - spot[1]) % ny
            return ((z - spot[0]) % nz) * nc + (c - spot[1]) % nc

        def hop(number, spot, child):
            if streams[number]["kind"] == "plane":
                return {"x": (x + child[0] - spot[0]) % nx, "y": (y + child[1] - spot[1]) % ny}
            return {"z": (z + child[0] - spot[0]) % nz, "c": (c + child[1] - spot[1]) % nc}

        def bulk(number, spot, child):
            ref = stores[number].at[origin_slot(number, spot)]
            k = ids[(number, child)]
            return pltpu.make_async_remote_copy(
                src_ref=ref,
                dst_ref=ref,
                send_sem=bulk_send.at[k],
                recv_sem=bulk_recv.at[k],
                device_id=hop(number, spot, child),
                device_id_type=MESH,
            )

        sent = []
        pending = list(order)

        def take(number, spot):
            if spot == (0, 0):
                if number < 3:
                    loads[number].wait()
                else:
                    loads[number + 2].wait()
            else:
                ref = stores[number].at[origin_slot(number, spot)]
                k = ids[(number, spot)]
                pltpu.make_async_copy(ref, ref, bulk_recv.at[k]).wait()
            for child in streams[number]["tree"][spot]:
                copy = bulk(number, spot, child)
                copy.start()
                sent.append(copy)
            if number == 2:
                slot = origin_slot(number, spot)
                piece = c_all[slot]
                at = pl.multiple_of(slot * t_cot, t_cot)
                c_t[:, pl.ds(at, t_cot)] = piece.T

        def advance(until):
            while pending and pending[0][0] <= until:
                _, number, spot = pending.pop(0)
                take(number, spot)

        def finish(numbers):
            while any(p[1] in numbers for p in pending):
                _, number, spot = pending.pop(0)
                take(number, spot)

        drains = []

        def exchange(k_sem, source, dest, group):
            count = plane if group == "plane" else cols
            mine = me_row if group == "plane" else me_col

            def one(k, carry):
                if group == "plane":
                    px, py = plane_peer(k)
                    where, slot = {"x": px, "y": py}, px * ny + py
                else:
                    pz, pc = col_peer(k)
                    where, slot = {"z": pz, "c": pc}, pz * nc + pc
                pltpu.make_async_remote_copy(
                    src_ref=source(slot),
                    dst_ref=dest.at[mine],
                    send_sem=small_send.at[k_sem],
                    recv_sem=small_recv.at[k_sem],
                    device_id=where,
                    device_id_type=MESH,
                ).start()
                return carry

            lax.fori_loop(1, count, one, 0)
            part = dest.at[pl.ds(0, count - 1)]
            drains.append(pltpu.make_async_copy(part, part, small_send.at[k_sem]))
            return pltpu.make_async_copy(part, part, small_recv.at[k_sem])

        advance(0.0)

        loads[3].wait()
        v3 = jnp.concatenate(split3(v[...]), axis=0)

        def fold3(t):
            return t[:RANK] + t[RANK : 2 * RANK] + t[2 * RANK :]

        lane = lax.broadcasted_iota(jnp.int32, (RANK, 2 * t_act), 1)
        here = (lane // t_act) == (me_row % 2)
        own_y, own_x = a_y[me_row], a_x[me_row]
        u_part = fold3(
            dot_nt(v3[:, :wy], jnp.concatenate([own_y, own_y], axis=0))
            + dot_nt(v3[:, wy:], jnp.concatenate([own_x, own_x], axis=0))
        )
        u_part = jnp.where(here, u_part, 0.0)
        for k in range(cols):
            u_s[k] = u_part[k * rpc : (k + 1) * rpc]
        u_r[me_col] = u_s[me_col]
        wait_u = exchange(0, lambda s: u_s.at[s], u_r, "col")
        loads[4].wait()
        v_part = fold3(dot_nt(v3, m[...]))
        for k in range(cols):
            v_s[k] = v_part[k * rpc : (k + 1) * rpc]
        v_r[me_col] = v_s[me_col]
        wait_v = exchange(1, lambda s: v_s.at[s], v_r, "col")
        advance(6.0)
        wait_u.wait()
        u_m[...] = jnp.sum(u_r[...], axis=0)
        u_g[me_row] = u_m[...]
        wait_ug = exchange(2, lambda s: u_m, u_g, "plane")
        advance(14.0)
        finish((2,))
        wait_ug.wait()
        u_full[...] = jnp.zeros_like(u_full)
        for k in range(plane // 2):
            u_full[0:rpc, k * 2 * t_act : (k + 1) * 2 * t_act] = u_g[2 * k] + u_g[2 * k + 1]
        u_rows = u_full.shape[0]
        u3 = jnp.concatenate([t.astype(F32) for t in split3(u_full[...])], axis=0).astype(BF16)
        from_gradient = dot_nt(u3, c_t[...])
        from_gradient = from_gradient[:u_rows] + from_gradient[u_rows : 2 * u_rows] + from_gradient[2 * u_rows :]
        wait_v.wait()
        l_s[...] = jnp.sum(v_r[...], axis=0) + grad_scale * from_gradient[:rpc]
        l_g[me_col] = l_s[...]
        wait_l = exchange(3, lambda s: l_s, l_g, "col")
        advance(20.0)
        wait_l.wait()
        for k in range(cols):
            left[k * rpc : (k + 1) * rpc, :] = l_g[k]
        whole_left = left[...]
        u_full[0:rpc, 0:rows] = l_s[...]
        g_part = dot_nt(u_full[:, 0:rows], whole_left, HIGHEST)
        g_s[...] = jnp.concatenate([g_part[:rpc], jnp.zeros((rpc, 128 - RANK), F32)], axis=1)
        g_r[me_row] = g_s[...]
        wait_g = exchange(4, lambda s: g_s, g_r, "plane")

        finish((0, 1))
        gathered_y = a_y[...].reshape(tokens, wy)
        gathered_x = a_x[...].reshape(tokens, wx)
        block = min(128, rows)

        def gradient_block(i, carry):
            at = pl.ds(pl.multiple_of(i * block, block), block)
            lhs = c_t[at, :]
            for cut, gathered in ((ky, gathered_y), (kx, gathered_x)):
                value = m[at, cut].astype(F32) + grad_scale * dot_nn(lhs, gathered)
                buf[at, cut] = value
                hi, lo = split2(value)
                b_hi[at, cut] = hi
                b_lo[at, cut] = lo
            return carry

        lax.fori_loop(0, rows // block, gradient_block, 0)
        wait_g.wait()
        g_m[...] = jnp.sum(g_r[...], axis=0)
        g_g[me_col] = g_m[...]
        wait_gg = exchange(5, lambda s: g_m, g_g, "col")
        advance(32.0)
        wait_gg.wait()
        for k in range(cols):
            gram[k * rpc : (k + 1) * rpc, :] = g_g[k]

        sub = lax.broadcasted_iota(jnp.int32, (RANK, 128), 0)
        lan = lax.broadcasted_iota(jnp.int32, (RANK, 128), 1)
        aug = jnp.where(lan - RANK == sub, 1.0, gram[...])
        for j in range(RANK - 1):
            row = aug[j : j + 1, :]
            col = aug[:, j : j + 1] / aug[j : j + 1, j : j + 1]
            aug = aug - jnp.where(sub > j, col * row, 0.0)
        pivot = jnp.sum(jnp.where(lan == sub, aug, 0.0), axis=1, keepdims=True)
        inverse = aug[:, RANK:] / jnp.sqrt(pivot)
        orth[...] = dot_nn(inverse, whole_left, HIGHEST)

        o_hi, o_lo = split2(orth[...])
        o_both = jnp.concatenate([o_hi, o_lo], axis=0)
        with_hi = dot_nn(o_both, b_hi[...])
        r_part = (with_hi[:RANK] + with_hi[RANK:]) + dot_nn(o_hi, b_lo[...])
        r_part = r_part.astype(BF16)
        for i in range(r_groups):
            for j in range(c_groups):
                r_s[i * c_groups + j] = r_part[16 * i : 16 * i + 16, j * c_width : (j + 1) * c_width]
        r_r[me_row] = r_s[me_row]
        wait_r = exchange(6, lambda s: r_s.at[s], r_r, "plane")
        finish((3, 4))

        loads[7].wait()
        per = n_out // n_next

        def product_block(i, carry):
            at = pl.ds(i * per, per)
            value = dot_nt(n_y[at].reshape(n_out, wy), w[:, :wy]) + dot_nt(n_x[at].reshape(n_out, wx), w[:, wy:])
            p_s[i % nc, i // nc] = (value * out_scale).astype(BF16)
            return carry

        lax.fori_loop(0, cols, product_block, 0)
        to_pair = pltpu.make_async_remote_copy(
            src_ref=p_s.at[1 - c],
            dst_ref=p_r,
            send_sem=small_send.at[7],
            recv_sem=small_recv.at[7],
            device_id={"c": 1 - c},
            device_id_type=MESH,
        )
        to_pair.start()
        wait_r.wait()
        r_m[...] = jnp.sum(r_r[...].astype(F32), axis=0).astype(BF16)
        r_g[me_row] = r_m[...]
        wait_rg = exchange(8, lambda s: r_m, r_g, "plane")
        to_pair.wait_recv()
        for k in range(nz):
            q_s[k] = (p_s[c, k].astype(F32) + p_r[k].astype(F32)).astype(BF16)

        def send_q(k, carry):
            pz = (z + k) % nz
            pltpu.make_async_remote_copy(
                src_ref=q_s.at[pz],
                dst_ref=q_r.at[z],
                send_sem=small_send.at[9],
                recv_sem=small_recv.at[9],
                device_id={"z": pz},
                device_id_type=MESH,
            ).start()
            return carry

        q_r[z] = q_s[z]
        lax.fori_loop(1, nz, send_q, 0)
        q_part = q_r.at[pl.ds(0, nz - 1)]
        wait_q = pltpu.make_async_copy(q_part, q_part, small_recv.at[9])
        drains.append(pltpu.make_async_copy(q_part, q_part, small_send.at[9]))
        wait_rg.wait()
        for i in range(r_groups):
            for j in range(c_groups):
                rmat[16 * i : 16 * i + 16, j * c_width : (j + 1) * c_width] = r_g[i * c_groups + j]
        right = rmat[...]
        right_f = right.astype(F32)
        squares = dot_nt(jnp.ones((8, width), F32), right_f * right_f, HIGHEST)
        s_s[...] = jnp.concatenate([squares, squares], axis=1)
        s_r[me_col] = s_s[...]
        wait_s = exchange(10, lambda s: s_s, s_r, "col")
        y_part = dot_nt(n_y[...].reshape(n_next * plane, wy), right[:, :wy])
        y_part = y_part + dot_nt(n_x[...].reshape(n_next * plane, wx), right[:, wy:])
        for k in range(cols):
            at = k * n_out
            y_s[k] = jnp.concatenate([y_part[at : at + half], y_part[at + half : at + n_out]], axis=1).astype(BF16)
        y_r[me_col] = y_s[me_col]
        wait_y = exchange(11, lambda s: y_s.at[s], y_r, "col")

        both = jnp.concatenate([right, right], axis=0)


        feed = dot_tn(o_both, both)
        m_out[...] = (buf[...] - feed_scale * feed).astype(BF16)

        wait_s.wait()
        total = jnp.sum(s_r[...], axis=0)[0:1]
        total = jnp.sum(jnp.where(lan == sub, total, 0.0), axis=1, keepdims=True)
        scale = 1.0 / jnp.sqrt(total + norm_eps)
        b_out[...] = right_f * scale
        scaled = orth[...] * (scale * step_scale)
        s_both = jnp.concatenate(split2(scaled), axis=0)
        w_out[...] = (w[...].astype(F32) - dot_tn(s_both, both)).astype(BF16)
        wait_y.wait()
        y_sum = jnp.sum(y_r[...].astype(F32), axis=0)
        y_sum = jnp.concatenate([y_sum[:, :RANK], y_sum[:, RANK:]], axis=0)
        low = dot_nn(y_sum * out_scale, scaled, HIGHEST)
        wait_q.wait()
        o_out[...] = (jnp.sum(q_r[...].astype(F32), axis=0) - low).astype(BF16)

        for copy in sent:
            copy.wait_send()
        to_pair.wait_send()
        for copy in drains:
            copy.wait()

    sub8 = max(8, rpc)
    vmem = pltpu.VMEM
    scratch = [
        vmem((plane, t_act, wy), BF16),
        vmem((plane, t_act, wx), BF16),
        vmem((cols, t_cot, rows), BF16),
        vmem((plane, n_next, wy), BF16),
        vmem((plane, n_next, wx), BF16),
        vmem((rows, tokens), BF16),
        vmem((rows, width), BF16),
        vmem((rows, width), BF16),
        vmem((RANK, width), F32),
        vmem((rows, width), F32),
        vmem((rows, width), BF16),
        vmem((rows, width), BF16),
        vmem((cols, rpc, 128), F32),
        vmem((cols, rpc, 128), F32),
        vmem((cols, rpc, rows), F32),
        vmem((cols, rpc, rows), F32),
        vmem((rpc, 128), F32),
        vmem((plane, rpc, 128), F32),
        vmem((sub8, tokens), F32),
        vmem((rpc, rows), F32),
        vmem((cols, rpc, rows), F32),
        vmem((RANK, rows), F32),
        vmem((rpc, 128), F32),
        vmem((plane, rpc, 128), F32),
        vmem((rpc, 128), F32),
        vmem((cols, rpc, 128), F32),
        vmem((RANK, 128), F32),
        vmem((RANK, rows), F32),
        vmem((plane, 16, c_width), BF16),
        vmem((plane, 16, c_width), BF16),
        vmem((16, c_width), BF16),
        vmem((plane, 16, c_width), BF16),
        vmem((RANK, width), BF16),
        vmem((nc, nz, n_out, rows), BF16),
        vmem((nz, n_out, rows), BF16),
        vmem((nz, n_out, rows), BF16),
        vmem((nz, n_out, rows), BF16),
        vmem((cols, half, 128), BF16),
        vmem((cols, half, 128), BF16),
        vmem((8, 128), F32),
        vmem((cols, 8, 128), F32),
        pltpu.SemaphoreType.DMA((n_bulk,)),
        pltpu.SemaphoreType.DMA((n_bulk,)),
        pltpu.SemaphoreType.DMA((12,)),
        pltpu.SemaphoreType.DMA((12,)),
        pltpu.SemaphoreType.DMA((8,)),
    ]
    return pl.pallas_call(
        kernel,
        out_shape=(
            jax.ShapeDtypeStruct((rows, width), BF16),
            jax.ShapeDtypeStruct((rows, width), BF16),
            jax.ShapeDtypeStruct((RANK, width), F32),
            jax.ShapeDtypeStruct((n_out, rows), BF16),
        ),
        in_specs=[pl.BlockSpec(memory_space=pl.ANY)] * 6,
        out_specs=[pl.BlockSpec(memory_space=pltpu.VMEM)] * 4,
        scratch_shapes=scratch,
        compiler_params=pltpu.CompilerParams(
            collective_id=0, has_side_effects=True, vmem_limit_bytes=60 * 1024 * 1024
        ),
    )


def solution(mesh, sizes=(4, 8, 8, 2)):
    torus = Mesh(mesh.devices.reshape(sizes), ("x", "y", "z", "c"))
    row, col = ("x", "y"), ("z", "c")

    def body(activations, cotangents, weights, momentum, right_basis, next_inputs):
        shapes = dict(act=activations.shape, cot=cotangents.shape, nxt=next_inputs.shape)
        return build(torus, shapes)(activations, cotangents, weights, momentum, right_basis, next_inputs)

    return jax.shard_map(
        body,
        mesh=torus,
        in_specs=(P(row, col), P(col, row), P(row, col), P(row, col), P(None, col), P(row, col)),
        out_specs=(P(row, col), P(row, col), P(None, col), P(col, row)),
        check_vma=False,
    )
```

```python
import heapq
import math

import jax
import jax.numpy as jnp
from jax import lax
from jax.experimental import pallas as pl
from jax.experimental.pallas import tpu as pltpu
from jax.sharding import Mesh
from jax.sharding import PartitionSpec as P

RANK = 64
MESH = pl.DeviceIdType.MESH
momentum_decay = 0.95
learn_rate = 0.3
norm_eps = 1e-06
F32 = jnp.float32
BF16 = jnp.bfloat16
HIGHEST = lax.Precision.HIGHEST

LATENCY = 2.5
RATE = 36e3
START_NEXT = 0.0
START_ACT = 8.0
T = (5.0, 13.0, 21.0, 26.0, 32.0, 38.0, 45.0, 53.0, 61.0)


def ring_paths(n, tie):
    reach = [d for d in range(1, (n + 1) // 2)]
    out = [d for d in reach] + [-d for d in reach]
    if n % 2 == 0:
        out.append(tie * (n // 2))
    return out


def sign(v):
    return (v > 0) - (v < 0)


def plane_tree(first, sizes):
    n1, n2 = sizes[first], sizes[1 - first]
    tree = {}

    def add(parent, child):
        tree.setdefault(parent, []).append(child)
        tree.setdefault(child, [])

    def place(d1, d2):
        return (d1, d2) if first == 0 else (d2, d1)

    tie = 1 if first == 0 else -1
    stem = sorted([0] + ring_paths(n1, tie), key=abs)
    for d1 in stem:
        if d1:
            add(place(d1 - sign(d1), 0), place(d1, 0))
    for d1 in stem:
        for d2 in sorted(ring_paths(n2, 1 if d1 % 2 else -1), key=abs):
            add(place(d1, d2 - sign(d2)), place(d1, d2))
    return tree


def planned(streams):
    free = {}
    queue = []
    order = []
    for number, stream in enumerate(streams):
        heapq.heappush(queue, (stream["start"], len(queue), False, number, stream["root"], None))
    count = len(queue)
    while queue:
        now, _, is_send, number, spot, child = heapq.heappop(queue)
        order.append((now, is_send, number, spot, child))
        if is_send:
            continue
        stream = streams[number]
        for child in stream["tree"][spot]:
            link = stream["link"](spot, child)
            cost = stream["bytes"] / (RATE if link != "pair" else 5e5)
            begin = max(now, free.get(link, 0.0))
            free[link] = begin + cost
            heapq.heappush(queue, (max(now, begin - cost), count, True, number, spot, child))
            heapq.heappush(queue, (free[link] + LATENCY, count + 1, False, number, child, None))
            count += 2
    return order


def split2(v):
    hi = v.astype(BF16)
    return hi, (v - hi.astype(F32)).astype(BF16)


def split3(v):
    hi = v.astype(BF16)
    rest = v - hi.astype(F32)
    mid = rest.astype(BF16)
    return hi, mid, (rest - mid.astype(F32)).astype(BF16)


def dot_nn(a, b, precision=None):
    return lax.dot_general(a, b, (((1,), (0,)), ((), ())), preferred_element_type=F32, precision=precision)


def dot_nt(a, b, precision=None):
    return lax.dot_general(a, b, (((1,), (1,)), ((), ())), preferred_element_type=F32, precision=precision)


def dot_tn(a, b, precision=None):
    return lax.dot_general(a, b, (((0,), (0,)), ((), ())), preferred_element_type=F32, precision=precision)


def build(mesh, shapes):
    nx, ny, nz, nc = (mesh.shape[a] for a in ("x", "y", "z", "c"))
    plane, cols = nx * ny, nz * nc
    t_act, width = shapes["act"]
    t_cot, rows = shapes["cot"]
    n_next = shapes["nxt"][0]
    tokens = t_act * plane
    n_out = n_next * plane // cols
    half = n_out // 2
    d_out, d_in = rows * plane, width * cols
    grad_scale = 1.0 / math.sqrt(tokens)
    out_scale = 1.0 / math.sqrt(d_in)
    step_scale = learn_rate * math.sqrt(d_out * d_in / RANK)
    feed_scale = 1.0 - momentum_decay
    wy = width * 5 // 8
    wx = width - wy
    rpc = RANK // cols
    r_groups = RANK // 16
    c_groups = plane // r_groups
    c_width = width // c_groups

    tree_y, tree_x = plane_tree(1, (nx, ny)), plane_tree(0, (nx, ny))

    def plane_link(a, b):
        return ("x", b[0] - a[0]) if a[1] == b[1] else ("y", b[1] - a[1])

    def cot_tree():
        tree = {}
        for d in sorted([0] + ring_paths(nz, 1), key=abs):
            if d:
                tree[(d - sign(d), 0)].append((d, 0))
            tree[(d, 0)] = [(d, 1)] if nc > 1 else []
            if nc > 1:
                tree[(d, 1)] = []
        return tree

    def cot_link(a, b):
        return "pair" if a[1] != b[1] else ("z", b[0] - a[0])

    streams = [
        dict(tree=tree_y, bytes=t_act * wy * 2, start=START_ACT, root=(0, 0), link=plane_link, kind="plane"),
        dict(tree=tree_x, bytes=t_act * wx * 2, start=START_ACT, root=(0, 0), link=plane_link, kind="plane"),
        dict(tree=cot_tree(), bytes=t_cot * rows * 2, start=0.0, root=(0, 0), link=cot_link, kind="col"),
        dict(tree=tree_y, bytes=n_next * wy * 2, start=START_NEXT, root=(0, 0), link=plane_link, kind="plane"),
        dict(tree=tree_x, bytes=n_next * wx * 2, start=START_NEXT, root=(0, 0), link=plane_link, kind="plane"),
    ]
    order = planned(streams)
    ids = {}
    for _, is_send, number, spot, _ in order:
        if not is_send and spot != (0, 0):
            ids[(number, spot)] = len(ids)
    n_bulk = len(ids)

    def kernel(
        act, cot, w_in, m_in, rb, nxt,
        w_out, m_out, b_out, o_out,
        a_y, a_x, c_all, n_y, n_x, c_t, w, m, v,
        s_m, l_pad, o_both,
        u_s, u_r, v_s, v_r, u_m, u_g, u_full, l_s, l_g, left, g_s, g_r, g_m, g_g, gram,
        orth, r_s, r_r, r_m, r_g, rmat,
        p_s, p_r, q_s, q_r, y_s, y_r, s_s, s_r,
        bulk_send, bulk_recv, small_send, small_recv, local_sem,
    ):
        x, y, z, c = (lax.axis_index(a) for a in ("x", "y", "z", "c"))
        me_row, me_col = x * ny + y, z * nc + c
        stores = [a_y, a_x, c_all, n_y, n_x]

        def local(src, dst, k):
            return pltpu.make_async_copy(src, dst, local_sem.at[k])

        ky, kx = pl.ds(0, wy), pl.ds(wy, wx)
        loads = [
            local(act.at[:, ky], a_y.at[me_row], 0),
            local(act.at[:, kx], a_x.at[me_row], 1),
            local(cot, c_all.at[me_col], 2),
            local(rb, v, 3),
            local(m_in, m, 4),
            local(nxt.at[:, ky], n_y.at[me_row], 5),
            local(nxt.at[:, kx], n_x.at[me_row], 6),
            local(w_in, w, 7),
        ]
        for copy in loads:
            copy.start()

        def plane_peer(k):
            return (x + k // ny) % nx, (y + k % ny) % ny

        def col_peer(k):
            return (z + k // nc) % nz, (c + k % nc) % nc

        barrier = pltpu.get_barrier_semaphore()

        def greet_plane(k, carry):
            px, py = plane_peer(k)
            pl.semaphore_signal(barrier, inc=1, device_id={"x": px, "y": py}, device_id_type=MESH)
            return carry

        def greet_col(k, carry):
            pz, pc = col_peer(k)
            pl.semaphore_signal(barrier, inc=1, device_id={"z": pz, "c": pc}, device_id_type=MESH)
            return carry

        lax.fori_loop(1, plane, greet_plane, 0)
        lax.fori_loop(1, cols, greet_col, 0)
        def origin_slot(number, spot):
            if streams[number]["kind"] == "plane":
                return ((x - spot[0]) % nx) * ny + (y - spot[1]) % ny
            return ((z - spot[0]) % nz) * nc + (c - spot[1]) % nc

        def hop(number, spot, child):
            if streams[number]["kind"] == "plane":
                return {"x": (x + child[0] - spot[0]) % nx, "y": (y + child[1] - spot[1]) % ny}
            return {"z": (z + child[0] - spot[0]) % nz, "c": (c + child[1] - spot[1]) % nc}

        def bulk(number, spot, child):
            ref = stores[number].at[origin_slot(number, spot)]
            k = ids[(number, child)]
            return pltpu.make_async_remote_copy(
                src_ref=ref,
                dst_ref=ref,
                send_sem=bulk_send.at[k],
                recv_sem=bulk_recv.at[k],
                device_id=hop(number, spot, child),
                device_id_type=MESH,
            )

        sent = []
        pending = list(order)

        def step():
            _, is_send, number, spot, child = pending.pop(0)
            if is_send:
                copy = bulk(number, spot, child)
                copy.start()
                sent.append(copy)
            elif spot == (0, 0):
                if number >= 2:
                    loads[number if number == 2 else number + 2].wait()
            else:
                ref = stores[number].at[origin_slot(number, spot)]
                pltpu.make_async_copy(ref, ref, bulk_recv.at[ids[(number, spot)]]).wait()

        def advance(until):
            while pending and pending[0][0] <= until:
                step()

        def finish(numbers):
            while any(p[2] in numbers for p in pending):
                step()

        drains = []

        def exchange(k_sem, source, dest, group):
            count = plane if group == "plane" else cols
            mine = me_row if group == "plane" else me_col

            def one(k, carry):
                if group == "plane":
                    px, py = plane_peer(k)
                    where, slot = {"x": px, "y": py}, px * ny + py
                else:
                    pz, pc = col_peer(k)
                    where, slot = {"z": pz, "c": pc}, pz * nc + pc
                pltpu.make_async_remote_copy(
                    src_ref=source(slot),
                    dst_ref=dest.at[mine],
                    send_sem=small_send.at[k_sem],
                    recv_sem=small_recv.at[k_sem],
                    device_id=where,
                    device_id_type=MESH,
                ).start()
                return carry

            lax.fori_loop(1, count, one, 0)
            part = dest.at[pl.ds(0, count - 1)]
            drains.append(pltpu.make_async_copy(part, part, small_send.at[k_sem]))
            return pltpu.make_async_copy(part, part, small_recv.at[k_sem])

        loads[3].wait()
        v3 = jnp.concatenate(split3(v[...]), axis=0)

        def fold3(t):
            return t[:RANK] + t[RANK : 2 * RANK] + t[2 * RANK :]

        lane = lax.broadcasted_iota(jnp.int32, (RANK, 2 * t_act), 1)
        here = (lane // t_act) == (me_row % 2)
        loads[0].wait()
        loads[1].wait()
        own_y, own_x = a_y[me_row], a_x[me_row]
        u_part = fold3(
            dot_nt(v3[:, :wy], jnp.concatenate([own_y, own_y], axis=0))
            + dot_nt(v3[:, wy:], jnp.concatenate([own_x, own_x], axis=0))
        )
        u_part = jnp.where(here, u_part, 0.0)
        for k in range(cols):
            u_s[k] = u_part[k * rpc : (k + 1) * rpc]
        u_r[me_col] = u_s[me_col]
        pl.semaphore_wait(barrier, plane - 1 + cols - 1)
        wait_u = exchange(0, lambda s: u_s.at[s], u_r, "col")
        advance(0.0)
        loads[4].wait()
        v_part = fold3(dot_nt(v3, m[...]))
        for k in range(cols):
            v_s[k] = v_part[k * rpc : (k + 1) * rpc]
        v_r[me_col] = v_s[me_col]
        wait_v = exchange(1, lambda s: v_s.at[s], v_r, "col")
        advance(T[0])
        wait_u.wait()
        u_m[...] = jnp.sum(u_r[...], axis=0)
        u_g[me_row] = u_m[...]
        wait_ug = exchange(2, lambda s: u_m, u_g, "plane")
        advance(T[1])
        finish((2,))
        wait_ug.wait()
        u_full[...] = jnp.zeros_like(u_full)
        for k in range(plane // 2):
            u_full[0:rpc, k * 2 * t_act : (k + 1) * 2 * t_act] = u_g[2 * k] + u_g[2 * k + 1]
        n8 = u_full.shape[0]

        def stacked(value):
            return jnp.concatenate([t.astype(F32) for t in split3(value)], axis=0).astype(BF16)

        def unstacked(t):
            return t[:n8] + t[n8 : 2 * n8] + t[2 * n8 :]

        cot_rows = c_all[...].reshape(tokens, rows)
        from_gradient = unstacked(dot_nn(stacked(u_full[...]), cot_rows))
        wait_v.wait()
        l_s[...] = jnp.sum(v_r[...], axis=0) + grad_scale * from_gradient[:rpc]
        l_g[me_col] = l_s[...]
        wait_l = exchange(3, lambda s: l_s, l_g, "col")
        advance(T[2])
        wait_l.wait()
        for k in range(cols):
            left[k * rpc : (k + 1) * rpc, :] = l_g[k]
        whole_left = left[...]

        l_pad[...] = jnp.zeros_like(l_pad)
        l_pad[0:rpc, :] = l_s[...]
        g_part = dot_nt(l_pad[...], whole_left, HIGHEST)[:rpc]
        z_part = unstacked(dot_nt(stacked(l_pad[...]), cot_rows))[:rpc] * grad_scale
        for k in range(plane):
            g_s[k] = jnp.concatenate([g_part, z_part[:, k * t_act : (k + 1) * t_act]], axis=1)
        g_r[me_row] = g_s[me_row]
        wait_g = exchange(4, lambda s: g_s.at[s], g_r, "plane")
        left_m = fold3(dot_nn(jnp.concatenate(split3(whole_left), axis=0), m[...]))
        s_m[...] = left_m
        advance(T[3])
        finish((3, 4))

        loads[7].wait()
        per = n_out // n_next

        def product_block(i, carry):
            at = pl.ds(i * per, per)
            value = dot_nt(n_y[at].reshape(n_out, wy), w[:, :wy]) + dot_nt(n_x[at].reshape(n_out, wx), w[:, wy:])
            p_s[i % nc, i // nc] = (value * out_scale).astype(BF16)
            return carry

        lax.fori_loop(0, cols, product_block, 0)
        to_pair = pltpu.make_async_remote_copy(
            src_ref=p_s.at[1 - c],
            dst_ref=p_r,
            send_sem=small_send.at[7],
            recv_sem=small_recv.at[7],
            device_id={"c": 1 - c},
            device_id_type=MESH,
        )
        to_pair.start()
        advance(T[4])
        wait_g.wait()
        g_m[...] = jnp.sum(g_r[...], axis=0)
        g_g[me_col] = g_m[...]
        wait_gg = exchange(5, lambda s: g_m, g_g, "col")

        def turned(i, carry):
            at = pl.multiple_of(i * t_cot, t_cot)
            c_t[:, pl.ds(at, t_cot)] = c_all[i].T
            return carry

        lax.fori_loop(0, cols, turned, 0)
        to_pair.wait_recv()
        for k in range(nz):
            q_s[k] = (p_s[c, k].astype(F32) + p_r[k].astype(F32)).astype(BF16)
        q_r[z] = q_s[z]
        advance(T[5])
        wait_gg.wait()

        def send_q(k, carry):
            pz = (z + k) % nz
            pltpu.make_async_remote_copy(
                src_ref=q_s.at[pz],
                dst_ref=q_r.at[z],
                send_sem=small_send.at[9],
                recv_sem=small_recv.at[9],
                device_id={"z": pz},
                device_id_type=MESH,
            ).start()
            return carry

        lax.fori_loop(1, nz, send_q, 0)
        q_part = q_r.at[pl.ds(0, nz - 1)]
        wait_q = pltpu.make_async_copy(q_part, q_part, small_recv.at[9])
        drains.append(pltpu.make_async_copy(q_part, q_part, small_send.at[9]))
        for k in range(cols):
            gram[k * rpc : (k + 1) * rpc, :] = g_g[k]
        gram_z = gram[...]
        z3 = jnp.concatenate(split3(gram_z[:, RANK:]), axis=0)
        s_m[:, ky] = s_m[:, ky] + fold3(dot_nn(z3, a_y[me_row]))
        s_m[:, kx] = s_m[:, kx] + fold3(dot_nn(z3, a_x[me_row]))

        sub = lax.broadcasted_iota(jnp.int32, (RANK, 128), 0)
        lan = lax.broadcasted_iota(jnp.int32, (RANK, 128), 1)
        aug = jnp.where(lan < RANK, gram_z, jnp.where(lan - RANK == sub, 1.0, 0.0))
        bands = [aug[8 * k : 8 * k + 8] for k in range(RANK // 8)]
        sub_band = lax.broadcasted_iota(jnp.int32, (8, 128), 0)
        for j in range(RANK - 1):
            top, at = divmod(j, 8)
            row = bands[top][at : at + 1, :]
            row_over = row * (1.0 / row[:, j : j + 1])
            for k in range((j + 1) // 8, RANK // 8):
                step_down = bands[k][:, j : j + 1] * row_over
                if k == top:
                    step_down = jnp.where(sub_band > at, step_down, 0.0)
                bands[k] = bands[k] - step_down
            if j % 16 == 15:
                advance(T[5] + (T[6] - T[5]) * (j + 1) / RANK)
        aug = jnp.concatenate(bands, axis=0)
        pivot = jnp.sum(jnp.where(lan == sub, aug, 0.0), axis=1, keepdims=True)
        inverse = aug[:, RANK:] / jnp.sqrt(pivot)

        r_part = dot_nn(inverse, s_m[...], HIGHEST).astype(BF16)
        for i in range(r_groups):
            for j in range(c_groups):
                r_s[i * c_groups + j] = r_part[16 * i : 16 * i + 16, j * c_width : (j + 1) * c_width]
        r_r[me_row] = r_s[me_row]
        wait_r = exchange(6, lambda s: r_s.at[s], r_r, "plane")
        orth[...] = dot_nn(inverse, whole_left, HIGHEST)
        o_both[...] = jnp.concatenate(split2(orth[...]), axis=0)
        advance(T[7])
        wait_r.wait()
        r_m[...] = jnp.sum(r_r[...].astype(F32), axis=0).astype(BF16)
        r_g[me_row] = r_m[...]
        wait_rg = exchange(8, lambda s: r_m, r_g, "plane")
        advance(T[8])
        wait_rg.wait()
        for i in range(r_groups):
            for j in range(c_groups):
                rmat[16 * i : 16 * i + 16, j * c_width : (j + 1) * c_width] = r_g[i * c_groups + j]
        right = rmat[...]
        right_f = right.astype(F32)
        squares = dot_nt(jnp.ones((8, width), F32), right_f * right_f, HIGHEST)
        s_s[...] = jnp.concatenate([squares, squares], axis=1)
        s_r[me_col] = s_s[...]
        wait_s = exchange(10, lambda s: s_s, s_r, "col")
        y_part = dot_nt(n_y[...].reshape(n_next * plane, wy), right[:, :wy])
        y_part = y_part + dot_nt(n_x[...].reshape(n_next * plane, wx), right[:, wy:])
        for k in range(cols):
            at = k * n_out
            y_s[k] = jnp.concatenate([y_part[at : at + half], y_part[at + half : at + n_out]], axis=1).astype(BF16)
        y_r[me_col] = y_s[me_col]
        wait_y = exchange(11, lambda s: y_s.at[s], y_r, "col")

        finish((0, 1))
        both = jnp.concatenate([right, right], axis=0)
        gathered_y = a_y[...].reshape(tokens, wy)
        gathered_x = a_x[...].reshape(tokens, wx)
        block = min(128, rows)

        def momentum_block(i, carry):
            at = pl.ds(pl.multiple_of(i * block, block), block)
            lhs, low_rank = c_t[at, :], o_both[:, at]
            for cut, gathered, part in ((ky, gathered_y, both[:, :wy]), (kx, gathered_x, both[:, wy:])):
                value = m[at, cut].astype(F32) + grad_scale * dot_nn(lhs, gathered)
                m_out[at, cut] = (value - feed_scale * dot_tn(low_rank, part)).astype(BF16)
            return carry

        lax.fori_loop(0, rows // block, momentum_block, 0)

        wait_s.wait()
        total = jnp.sum(s_r[...], axis=0)[0:1]
        total = jnp.sum(jnp.where(lan == sub, total, 0.0), axis=1, keepdims=True)
        scale = 1.0 / jnp.sqrt(total + norm_eps)
        b_out[...] = right_f * scale
        scaled = orth[...] * (scale * step_scale)
        s_both = jnp.concatenate(split2(scaled), axis=0)
        w_out[...] = (w[...].astype(F32) - dot_tn(s_both, both)).astype(BF16)
        wait_y.wait()
        y_sum = jnp.sum(y_r[...].astype(F32), axis=0)
        y_sum = jnp.concatenate([y_sum[:, :RANK], y_sum[:, RANK:]], axis=0)
        low = dot_nn(y_sum * out_scale, scaled, HIGHEST)
        wait_q.wait()
        o_out[...] = (jnp.sum(q_r[...].astype(F32), axis=0) - low).astype(BF16)

        for copy in sent:
            copy.wait_send()
        to_pair.wait_send()
        for copy in drains:
            copy.wait()

    sub8 = max(8, rpc)
    vmem = pltpu.VMEM
    scratch = [
        vmem((plane, t_act, wy), BF16),
        vmem((plane, t_act, wx), BF16),
        vmem((cols, t_cot, rows), BF16),
        vmem((plane, n_next, wy), BF16),
        vmem((plane, n_next, wx), BF16),
        vmem((rows, tokens), BF16),
        vmem((rows, width), BF16),
        vmem((rows, width), BF16),
        vmem((RANK, width), F32),
        vmem((RANK, width), F32),
        vmem((sub8, rows), F32),
        vmem((2 * RANK, rows), BF16),
        vmem((cols, rpc, 128), F32),
        vmem((cols, rpc, 128), F32),
        vmem((cols, rpc, rows), F32),
        vmem((cols, rpc, rows), F32),
        vmem((rpc, 128), F32),
        vmem((plane, rpc, 128), F32),
        vmem((sub8, tokens), F32),
        vmem((rpc, rows), F32),
        vmem((cols, rpc, rows), F32),
        vmem((RANK, rows), F32),
        vmem((plane, rpc, 128), F32),
        vmem((plane, rpc, 128), F32),
        vmem((rpc, 128), F32),
        vmem((cols, rpc, 128), F32),
        vmem((RANK, 128), F32),
        vmem((RANK, rows), F32),
        vmem((plane, 16, c_width), BF16),
        vmem((plane, 16, c_width), BF16),
        vmem((16, c_width), BF16),
        vmem((plane, 16, c_width), BF16),
        vmem((RANK, width), BF16),
        vmem((nc, nz, n_out, rows), BF16),
        vmem((nz, n_out, rows), BF16),
        vmem((nz, n_out, rows), BF16),
        vmem((nz, n_out, rows), BF16),
        vmem((cols, half, 128), BF16),
        vmem((cols, half, 128), BF16),
        vmem((8, 128), F32),
        vmem((cols, 8, 128), F32),
        pltpu.SemaphoreType.DMA((n_bulk,)),
        pltpu.SemaphoreType.DMA((n_bulk,)),
        pltpu.SemaphoreType.DMA((12,)),
        pltpu.SemaphoreType.DMA((12,)),
        pltpu.SemaphoreType.DMA((8,)),
    ]
    return pl.pallas_call(
        kernel,
        out_shape=(
            jax.ShapeDtypeStruct((rows, width), BF16),
            jax.ShapeDtypeStruct((rows, width), BF16),
            jax.ShapeDtypeStruct((RANK, width), F32),
            jax.ShapeDtypeStruct((n_out, rows), BF16),
        ),
        in_specs=[pl.BlockSpec(memory_space=pltpu.HBM)] * 6,
        out_specs=[pl.BlockSpec(memory_space=pltpu.VMEM)] * 4,
        scratch_shapes=scratch,
        compiler_params=pltpu.CompilerParams(
            collective_id=0, has_side_effects=True, vmem_limit_bytes=60 * 1024 * 1024
        ),
    )


def placed(values):
    count = len(values)

    def kernel(*refs):
        sems = refs[-1]
        copies = [pltpu.make_async_copy(refs[k], refs[count + k], sems.at[k]) for k in range(count)]
        for copy in copies:
            copy.start()
        for copy in copies:
            copy.wait()

    return pl.pallas_call(
        kernel,
        out_shape=tuple(jax.ShapeDtypeStruct(v.shape, v.dtype) for v in values),
        in_specs=[pl.BlockSpec(memory_space=pltpu.VMEM)] * count,
        out_specs=[pl.BlockSpec(memory_space=pl.ANY)] * count,
        scratch_shapes=[pltpu.SemaphoreType.DMA((count,))],
        compiler_params=pltpu.CompilerParams(vmem_limit_bytes=8 * 1024 * 1024),
    )(*values)


def solution(mesh, sizes=(4, 8, 8, 2)):
    torus = Mesh(mesh.devices.reshape(sizes), ("x", "y", "z", "c"))
    row, col = ("x", "y"), ("z", "c")

    def body(activations, cotangents, weights, momentum, right_basis, next_inputs):
        shapes = dict(act=activations.shape, cot=cotangents.shape, nxt=next_inputs.shape)
        results = build(torus, shapes)(activations, cotangents, weights, momentum, right_basis, next_inputs)
        return placed(results)

    return jax.shard_map(
        body,
        mesh=torus,
        in_specs=(P(row, col), P(col, row), P(row, col), P(row, col), P(None, col), P(row, col)),
        out_specs=(P(row, col), P(row, col), P(None, col), P(col, row)),
        check_vma=False,
    )
```

```python
import heapq
import math

import jax
import jax.numpy as jnp
from jax import lax
from jax.experimental import pallas as pl
from jax.experimental.pallas import tpu as pltpu
from jax.sharding import Mesh
from jax.sharding import PartitionSpec as P

RANK = 64
MESH = pl.DeviceIdType.MESH
momentum_decay = 0.95
learn_rate = 0.3
norm_eps = 1e-06
F32 = jnp.float32
BF16 = jnp.bfloat16
HIGHEST = lax.Precision.HIGHEST

LATENCY = 2.5
RATE = 36e3
START_NEXT = 0.0
START_ACT = 8.0
T = (5.0, 13.0, 21.0, 26.0, 32.0, 38.0, 45.0, 53.0, 61.0)


def ring_paths(n, tie):
    reach = [d for d in range(1, (n + 1) // 2)]
    out = [d for d in reach] + [-d for d in reach]
    if n % 2 == 0:
        out.append(tie * (n // 2))
    return out


def sign(v):
    return (v > 0) - (v < 0)


def plane_tree(first, sizes):
    n1, n2 = sizes[first], sizes[1 - first]
    tree = {}

    def add(parent, child):
        tree.setdefault(parent, []).append(child)
        tree.setdefault(child, [])

    def place(d1, d2):
        return (d1, d2) if first == 0 else (d2, d1)

    tie = 1 if first == 0 else -1
    stem = sorted([0] + ring_paths(n1, tie), key=abs)
    for d1 in stem:
        if d1:
            add(place(d1 - sign(d1), 0), place(d1, 0))
    for d1 in stem:
        for d2 in sorted(ring_paths(n2, 1 if d1 % 2 else -1), key=abs):
            add(place(d1, d2 - sign(d2)), place(d1, d2))
    return tree


def planned(streams):
    free = {}
    queue = []
    order = []
    for number, stream in enumerate(streams):
        heapq.heappush(queue, (stream["start"], len(queue), False, number, stream["root"], None))
    count = len(queue)
    while queue:
        now, _, is_send, number, spot, child = heapq.heappop(queue)
        order.append((now, is_send, number, spot, child))
        if is_send:
            continue
        stream = streams[number]
        for child in stream["tree"][spot]:
            link = stream["link"](spot, child)
            cost = stream["bytes"] / (RATE if link != "pair" else 5e5)
            begin = max(now, free.get(link, 0.0))
            free[link] = begin + cost
            heapq.heappush(queue, (max(now, begin - cost), count, True, number, spot, child))
            heapq.heappush(queue, (free[link] + LATENCY, count + 1, False, number, child, None))
            count += 2
    return order


def split2(v):
    hi = v.astype(BF16)
    return hi, (v - hi.astype(F32)).astype(BF16)


def split3(v):
    hi = v.astype(BF16)
    rest = v - hi.astype(F32)
    mid = rest.astype(BF16)
    return hi, mid, (rest - mid.astype(F32)).astype(BF16)


def dot_nn(a, b, precision=None):
    return lax.dot_general(a, b, (((1,), (0,)), ((), ())), preferred_element_type=F32, precision=precision)


def dot_nt(a, b, precision=None):
    return lax.dot_general(a, b, (((1,), (1,)), ((), ())), preferred_element_type=F32, precision=precision)


def dot_tn(a, b, precision=None):
    return lax.dot_general(a, b, (((0,), (0,)), ((), ())), preferred_element_type=F32, precision=precision)


def build(mesh, shapes):
    nx, ny, nz, nc = (mesh.shape[a] for a in ("x", "y", "z", "c"))
    plane, cols = nx * ny, nz * nc
    t_act, width = shapes["act"]
    t_cot, rows = shapes["cot"]
    n_next = shapes["nxt"][0]
    tokens = t_act * plane
    n_out = n_next * plane // cols
    half = n_out // 2
    d_out, d_in = rows * plane, width * cols
    grad_scale = 1.0 / math.sqrt(tokens)
    out_scale = 1.0 / math.sqrt(d_in)
    step_scale = learn_rate * math.sqrt(d_out * d_in / RANK)
    feed_scale = 1.0 - momentum_decay
    wy = width * 5 // 8
    wx = width - wy
    rpc = RANK // cols
    r_groups = RANK // 16
    c_groups = plane // r_groups
    c_width = width // c_groups

    tree_y, tree_x = plane_tree(1, (nx, ny)), plane_tree(0, (nx, ny))

    def plane_link(a, b):
        return ("x", b[0] - a[0]) if a[1] == b[1] else ("y", b[1] - a[1])

    def cot_tree():
        tree = {}
        for d in sorted([0] + ring_paths(nz, 1), key=abs):
            if d:
                tree[(d - sign(d), 0)].append((d, 0))
            tree[(d, 0)] = [(d, 1)] if nc > 1 else []
            if nc > 1:
                tree[(d, 1)] = []
        return tree

    def cot_link(a, b):
        return "pair" if a[1] != b[1] else ("z", b[0] - a[0])

    streams = [
        dict(tree=tree_y, bytes=t_act * wy * 2, start=START_ACT, root=(0, 0), link=plane_link, kind="plane"),
        dict(tree=tree_x, bytes=t_act * wx * 2, start=START_ACT, root=(0, 0), link=plane_link, kind="plane"),
        dict(tree=cot_tree(), bytes=t_cot * rows * 2, start=0.0, root=(0, 0), link=cot_link, kind="col"),
        dict(tree=tree_y, bytes=n_next * wy * 2, start=START_NEXT, root=(0, 0), link=plane_link, kind="plane"),
        dict(tree=tree_x, bytes=n_next * wx * 2, start=START_NEXT, root=(0, 0), link=plane_link, kind="plane"),
    ]
    order = planned(streams)
    ids = {}
    for _, is_send, number, spot, _ in order:
        if not is_send and spot != (0, 0):
            ids[(number, spot)] = len(ids)
    n_bulk = len(ids)

    def kernel(
        act, cot, w_in, m_in, rb, nxt,
        w_out, m_out, b_out, o_out,
        a_y, a_x, c_all, n_y, n_x, c_t, w, m, v,
        s_m, l_pad, o_both,
        u_s, u_r, v_s, v_r, u_m, u_g, u_full, l_s, l_g, left, g_s, g_r, g_m, g_g, gram,
        orth, r_s, r_r, r_m, r_g, rmat,
        p_s, p_r, q_s, q_r, y_s, y_r, s_s, s_r,
        bulk_send, bulk_recv, small_send, small_recv, local_sem,
    ):
        x, y, z, c = (lax.axis_index(a) for a in ("x", "y", "z", "c"))
        me_row, me_col = x * ny + y, z * nc + c
        stores = [a_y, a_x, c_all, n_y, n_x]

        def local(src, dst, k):
            return pltpu.make_async_copy(src, dst, local_sem.at[k])

        ky, kx = pl.ds(0, wy), pl.ds(wy, wx)
        loads = [
            local(act.at[:, ky], a_y.at[me_row], 0),
            local(act.at[:, kx], a_x.at[me_row], 1),
            local(cot, c_all.at[me_col], 2),
            local(rb, v, 3),
            local(m_in, m, 4),
            local(nxt.at[:, ky], n_y.at[me_row], 5),
            local(nxt.at[:, kx], n_x.at[me_row], 6),
            local(w_in, w, 7),
        ]
        for copy in loads:
            copy.start()

        def plane_peer(k):
            return (x + k // ny) % nx, (y + k % ny) % ny

        def col_peer(k):
            return (z + k // nc) % nz, (c + k % nc) % nc

        barrier = pltpu.get_barrier_semaphore()

        def greet_plane(k, carry):
            px, py = plane_peer(k)
            pl.semaphore_signal(barrier, inc=1, device_id={"x": px, "y": py}, device_id_type=MESH)
            return carry

        def greet_col(k, carry):
            pz, pc = col_peer(k)
            pl.semaphore_signal(barrier, inc=1, device_id={"z": pz, "c": pc}, device_id_type=MESH)
            return carry

        lax.fori_loop(1, plane, greet_plane, 0)
        lax.fori_loop(1, cols, greet_col, 0)
        def origin_slot(number, spot):
            if streams[number]["kind"] == "plane":
                return ((x - spot[0]) % nx) * ny + (y - spot[1]) % ny
            return ((z - spot[0]) % nz) * nc + (c - spot[1]) % nc

        def hop(number, spot, child):
            if streams[number]["kind"] == "plane":
                return {"x": (x + child[0] - spot[0]) % nx, "y": (y + child[1] - spot[1]) % ny}
            return {"z": (z + child[0] - spot[0]) % nz, "c": (c + child[1] - spot[1]) % nc}

        def bulk(number, spot, child):
            ref = stores[number].at[origin_slot(number, spot)]
            k = ids[(number, child)]
            return pltpu.make_async_remote_copy(
                src_ref=ref,
                dst_ref=ref,
                send_sem=bulk_send.at[k],
                recv_sem=bulk_recv.at[k],
                device_id=hop(number, spot, child),
                device_id_type=MESH,
            )

        sent = []
        pending = list(order)

        def step():
            _, is_send, number, spot, child = pending.pop(0)
            if is_send:
                copy = bulk(number, spot, child)
                copy.start()
                sent.append(copy)
            elif spot == (0, 0):
                if number >= 2:
                    loads[number if number == 2 else number + 2].wait()
            else:
                ref = stores[number].at[origin_slot(number, spot)]
                pltpu.make_async_copy(ref, ref, bulk_recv.at[ids[(number, spot)]]).wait()

        def advance(until):
            while pending and pending[0][0] <= until:
                step()

        def finish(numbers):
            while any(p[2] in numbers for p in pending):
                step()

        drains = []

        def exchange(k_sem, source, dest, group):
            count = plane if group == "plane" else cols
            mine = me_row if group == "plane" else me_col

            def one(k, carry):
                if group == "plane":
                    px, py = plane_peer(k)
                    where, slot = {"x": px, "y": py}, px * ny + py
                else:
                    pz, pc = col_peer(k)
                    where, slot = {"z": pz, "c": pc}, pz * nc + pc
                pltpu.make_async_remote_copy(
                    src_ref=source(slot),
                    dst_ref=dest.at[mine],
                    send_sem=small_send.at[k_sem],
                    recv_sem=small_recv.at[k_sem],
                    device_id=where,
                    device_id_type=MESH,
                ).start()
                return carry

            lax.fori_loop(1, count, one, 0)
            part = dest.at[pl.ds(0, count - 1)]
            drains.append(pltpu.make_async_copy(part, part, small_send.at[k_sem]))
            return pltpu.make_async_copy(part, part, small_recv.at[k_sem])

        loads[3].wait()
        v3 = jnp.concatenate(split3(v[...]), axis=0)

        def fold3(t):
            return t[:RANK] + t[RANK : 2 * RANK] + t[2 * RANK :]

        lane = lax.broadcasted_iota(jnp.int32, (RANK, 2 * t_act), 1)
        here = (lane // t_act) == (me_row % 2)
        loads[0].wait()
        loads[1].wait()
        own_y, own_x = a_y[me_row], a_x[me_row]
        u_part = fold3(
            dot_nt(v3[:, :wy], jnp.concatenate([own_y, own_y], axis=0))
            + dot_nt(v3[:, wy:], jnp.concatenate([own_x, own_x], axis=0))
        )
        u_part = jnp.where(here, u_part, 0.0)
        for k in range(cols):
            u_s[k] = u_part[k * rpc : (k + 1) * rpc]
        u_r[me_col] = u_s[me_col]
        pl.semaphore_wait(barrier, plane - 1 + cols - 1)
        wait_u = exchange(0, lambda s: u_s.at[s], u_r, "col")
        advance(0.0)
        loads[4].wait()
        v_part = fold3(dot_nt(v3, m[...]))
        for k in range(cols):
            v_s[k] = v_part[k * rpc : (k + 1) * rpc]
        v_r[me_col] = v_s[me_col]
        wait_v = exchange(1, lambda s: v_s.at[s], v_r, "col")
        advance(T[0])
        wait_u.wait()
        u_m[...] = jnp.sum(u_r[...], axis=0)
        u_g[me_row] = u_m[...]
        wait_ug = exchange(2, lambda s: u_m, u_g, "plane")
        advance(T[1])
        finish((2,))
        wait_ug.wait()
        u_full[...] = jnp.zeros_like(u_full)
        for k in range(plane // 2):
            u_full[0:rpc, k * 2 * t_act : (k + 1) * 2 * t_act] = u_g[2 * k] + u_g[2 * k + 1]
        n8 = u_full.shape[0]

        def stacked(value):
            return jnp.concatenate([t.astype(F32) for t in split3(value)], axis=0).astype(BF16)

        def unstacked(t):
            return t[:n8] + t[n8 : 2 * n8] + t[2 * n8 :]

        cot_rows = c_all[...].reshape(tokens, rows)
        from_gradient = unstacked(dot_nn(stacked(u_full[...]), cot_rows))
        wait_v.wait()
        l_s[...] = jnp.sum(v_r[...], axis=0) + grad_scale * from_gradient[:rpc]
        l_g[me_col] = l_s[...]
        wait_l = exchange(3, lambda s: l_s, l_g, "col")
        advance(T[2])
        wait_l.wait()
        for k in range(cols):
            left[k * rpc : (k + 1) * rpc, :] = l_g[k]
        whole_left = left[...]

        l_pad[...] = jnp.zeros_like(l_pad)
        l_pad[0:rpc, :] = l_s[...]
        g_part = dot_nt(l_pad[...], whole_left, HIGHEST)[:rpc]
        z_part = unstacked(dot_nt(stacked(l_pad[...]), cot_rows))[:rpc] * grad_scale
        for k in range(plane):
            g_s[k] = jnp.concatenate([g_part, z_part[:, k * t_act : (k + 1) * t_act]], axis=1)
        g_r[me_row] = g_s[me_row]
        wait_g = exchange(4, lambda s: g_s.at[s], g_r, "plane")
        left_m = fold3(dot_nn(jnp.concatenate(split3(whole_left), axis=0), m[...]))
        s_m[...] = left_m
        advance(T[3])
        finish((3, 4))

        loads[7].wait()
        per = n_out // n_next

        def product_block(i, carry):
            at = pl.ds(i * 4 * per, 4 * per)
            value = dot_nt(n_y[at].reshape(4 * n_out, wy), w[:, :wy])
            value = value + dot_nt(n_x[at].reshape(4 * n_out, wx), w[:, wy:])
            for j in range(4):
                p_s[j % nc, i * (4 // nc) + j // nc] = (value[j * n_out : (j + 1) * n_out] * out_scale).astype(BF16)
            return carry

        lax.fori_loop(0, cols // 4, product_block, 0)
        to_pair = pltpu.make_async_remote_copy(
            src_ref=p_s.at[1 - c],
            dst_ref=p_r,
            send_sem=small_send.at[7],
            recv_sem=small_recv.at[7],
            device_id={"c": 1 - c},
            device_id_type=MESH,
        )
        to_pair.start()
        advance(T[4])
        wait_g.wait()
        g_m[...] = jnp.sum(g_r[...], axis=0)
        g_g[me_col] = g_m[...]
        wait_gg = exchange(5, lambda s: g_m, g_g, "col")

        def turned(i, carry):
            at = pl.multiple_of(i * t_cot, t_cot)
            c_t[:, pl.ds(at, t_cot)] = c_all[i].T
            return carry

        lax.fori_loop(0, cols, turned, 0)
        to_pair.wait_recv()
        for k in range(nz):
            q_s[k] = (p_s[c, k].astype(F32) + p_r[k].astype(F32)).astype(BF16)
        q_r[z] = q_s[z]
        advance(T[5])
        wait_gg.wait()

        def send_q(k, carry):
            pz = (z + k) % nz
            pltpu.make_async_remote_copy(
                src_ref=q_s.at[pz],
                dst_ref=q_r.at[z],
                send_sem=small_send.at[9],
                recv_sem=small_recv.at[9],
                device_id={"z": pz},
                device_id_type=MESH,
            ).start()
            return carry

        lax.fori_loop(1, nz, send_q, 0)
        q_part = q_r.at[pl.ds(0, nz - 1)]
        wait_q = pltpu.make_async_copy(q_part, q_part, small_recv.at[9])
        drains.append(pltpu.make_async_copy(q_part, q_part, small_send.at[9]))
        for k in range(cols):
            gram[k * rpc : (k + 1) * rpc, :] = g_g[k]
        gram_z = gram[...]
        z3 = jnp.concatenate(split3(gram_z[:, RANK:]), axis=0)
        s_m[:, ky] = s_m[:, ky] + fold3(dot_nn(z3, a_y[me_row]))
        s_m[:, kx] = s_m[:, kx] + fold3(dot_nn(z3, a_x[me_row]))

        sub = lax.broadcasted_iota(jnp.int32, (RANK, 128), 0)
        lan = lax.broadcasted_iota(jnp.int32, (RANK, 128), 1)
        aug = jnp.where(lan < RANK, gram_z, jnp.where(lan - RANK == sub, 1.0, 0.0))
        bands = [aug[8 * k : 8 * k + 8] for k in range(RANK // 8)]
        sub_band = lax.broadcasted_iota(jnp.int32, (8, 128), 0)
        for j in range(RANK - 1):
            top, at = divmod(j, 8)
            row = bands[top][at : at + 1, :]
            row_over = row * (1.0 / row[:, j : j + 1])
            for k in range((j + 1) // 8, RANK // 8):
                step_down = bands[k][:, j : j + 1] * row_over
                if k == top:
                    step_down = jnp.where(sub_band > at, step_down, 0.0)
                bands[k] = bands[k] - step_down
            if j % 16 == 15:
                advance(T[5] + (T[6] - T[5]) * (j + 1) / RANK)
        aug = jnp.concatenate(bands, axis=0)
        pivot = jnp.sum(jnp.where(lan == sub, aug, 0.0), axis=1, keepdims=True)
        inverse = aug[:, RANK:] / jnp.sqrt(pivot)

        r_part = dot_nn(inverse, s_m[...], HIGHEST).astype(BF16)
        for i in range(r_groups):
            for j in range(c_groups):
                r_s[i * c_groups + j] = r_part[16 * i : 16 * i + 16, j * c_width : (j + 1) * c_width]
        r_r[me_row] = r_s[me_row]
        wait_r = exchange(6, lambda s: r_s.at[s], r_r, "plane")
        orth[...] = dot_nn(inverse, whole_left, HIGHEST)
        o_both[...] = jnp.concatenate(split2(orth[...]), axis=0)
        advance(T[7])
        wait_r.wait()
        r_m[...] = jnp.sum(r_r[...].astype(F32), axis=0).astype(BF16)
        r_g[me_row] = r_m[...]
        wait_rg = exchange(8, lambda s: r_m, r_g, "plane")
        advance(T[8])
        wait_rg.wait()
        for i in range(r_groups):
            for j in range(c_groups):
                rmat[16 * i : 16 * i + 16, j * c_width : (j + 1) * c_width] = r_g[i * c_groups + j]
        right = rmat[...]
        right_f = right.astype(F32)
        squares = dot_nt(jnp.ones((8, width), F32), right_f * right_f, HIGHEST)
        s_s[...] = jnp.concatenate([squares, squares], axis=1)
        s_r[me_col] = s_s[...]
        wait_s = exchange(10, lambda s: s_s, s_r, "col")
        y_part = dot_nt(n_y[...].reshape(n_next * plane, wy), right[:, :wy])
        y_part = y_part + dot_nt(n_x[...].reshape(n_next * plane, wx), right[:, wy:])
        for k in range(cols):
            at = k * n_out
            y_s[k] = jnp.concatenate([y_part[at : at + half], y_part[at + half : at + n_out]], axis=1).astype(BF16)
        y_r[me_col] = y_s[me_col]
        wait_y = exchange(11, lambda s: y_s.at[s], y_r, "col")

        finish((0, 1))
        both = jnp.concatenate([right, right], axis=0)
        gathered_y = a_y[...].reshape(tokens, wy)
        gathered_x = a_x[...].reshape(tokens, wx)
        block = min(128, rows)

        def momentum_block(i, carry):
            at = pl.ds(pl.multiple_of(i * block, block), block)
            lhs, low_rank = c_t[at, :], o_both[:, at]
            for cut, gathered, part in ((ky, gathered_y, both[:, :wy]), (kx, gathered_x, both[:, wy:])):
                value = m[at, cut].astype(F32) + grad_scale * dot_nn(lhs, gathered)
                m_out[at, cut] = (value - feed_scale * dot_tn(low_rank, part)).astype(BF16)
            return carry

        lax.fori_loop(0, rows // block, momentum_block, 0)

        wait_s.wait()
        total = jnp.sum(s_r[...], axis=0)[0:1]
        total = jnp.sum(jnp.where(lan == sub, total, 0.0), axis=1, keepdims=True)
        scale = 1.0 / jnp.sqrt(total + norm_eps)
        b_out[...] = right_f * scale
        scaled = orth[...] * (scale * step_scale)
        s_both = jnp.concatenate(split2(scaled), axis=0)
        w_out[...] = (w[...].astype(F32) - dot_tn(s_both, both)).astype(BF16)
        wait_y.wait()
        y_sum = jnp.sum(y_r[...].astype(F32), axis=0)
        y_sum = jnp.concatenate([y_sum[:, :RANK], y_sum[:, RANK:]], axis=0)
        low = dot_nn(y_sum * out_scale, scaled, HIGHEST)
        wait_q.wait()
        o_out[...] = (jnp.sum(q_r[...].astype(F32), axis=0) - low).astype(BF16)

        for copy in sent:
            copy.wait_send()
        to_pair.wait_send()
        for copy in drains:
            copy.wait()

    sub8 = max(8, rpc)
    vmem = pltpu.VMEM
    scratch = [
        vmem((plane, t_act, wy), BF16),
        vmem((plane, t_act, wx), BF16),
        vmem((cols, t_cot, rows), BF16),
        vmem((plane, n_next, wy), BF16),
        vmem((plane, n_next, wx), BF16),
        vmem((rows, tokens), BF16),
        vmem((rows, width), BF16),
        vmem((rows, width), BF16),
        vmem((RANK, width), F32),
        vmem((RANK, width), F32),
        vmem((sub8, rows), F32),
        vmem((2 * RANK, rows), BF16),
        vmem((cols, rpc, 128), F32),
        vmem((cols, rpc, 128), F32),
        vmem((cols, rpc, rows), F32),
        vmem((cols, rpc, rows), F32),
        vmem((rpc, 128), F32),
        vmem((plane, rpc, 128), F32),
        vmem((sub8, tokens), F32),
        vmem((rpc, rows), F32),
        vmem((cols, rpc, rows), F32),
        vmem((RANK, rows), F32),
        vmem((plane, rpc, 128), F32),
        vmem((plane, rpc, 128), F32),
        vmem((rpc, 128), F32),
        vmem((cols, rpc, 128), F32),
        vmem((RANK, 128), F32),
        vmem((RANK, rows), F32),
        vmem((plane, 16, c_width), BF16),
        vmem((plane, 16, c_width), BF16),
        vmem((16, c_width), BF16),
        vmem((plane, 16, c_width), BF16),
        vmem((RANK, width), BF16),
        vmem((nc, nz, n_out, rows), BF16),
        vmem((nz, n_out, rows), BF16),
        vmem((nz, n_out, rows), BF16),
        vmem((nz, n_out, rows), BF16),
        vmem((cols, half, 128), BF16),
        vmem((cols, half, 128), BF16),
        vmem((8, 128), F32),
        vmem((cols, 8, 128), F32),
        pltpu.SemaphoreType.DMA((n_bulk,)),
        pltpu.SemaphoreType.DMA((n_bulk,)),
        pltpu.SemaphoreType.DMA((12,)),
        pltpu.SemaphoreType.DMA((12,)),
        pltpu.SemaphoreType.DMA((8,)),
    ]
    return pl.pallas_call(
        kernel,
        out_shape=(
            jax.ShapeDtypeStruct((rows, width), BF16),
            jax.ShapeDtypeStruct((rows, width), BF16),
            jax.ShapeDtypeStruct((RANK, width), F32),
            jax.ShapeDtypeStruct((n_out, rows), BF16),
        ),
        in_specs=[pl.BlockSpec(memory_space=pltpu.HBM)] * 6,
        out_specs=[pl.BlockSpec(memory_space=pltpu.VMEM)] * 4,
        scratch_shapes=scratch,
        compiler_params=pltpu.CompilerParams(
            collective_id=0, has_side_effects=True, vmem_limit_bytes=60 * 1024 * 1024
        ),
    )


def placed(values):
    count = len(values)

    def kernel(*refs):
        stage, sems = refs[2 * count : 3 * count], refs[-1]
        taken = [pltpu.make_async_copy(refs[k], stage[k], sems.at[0, k]) for k in range(count)]
        given = [pltpu.make_async_copy(stage[k], refs[count + k], sems.at[1, k]) for k in range(count)]
        for copy in taken:
            copy.start()
        for k in range(count):
            taken[k].wait()
            given[k].start()
        for copy in given:
            copy.wait()

    return pl.pallas_call(
        kernel,
        out_shape=tuple(jax.ShapeDtypeStruct(v.shape, v.dtype) for v in values),
        in_specs=[pl.BlockSpec(memory_space=pl.ANY)] * count,
        out_specs=[pl.BlockSpec(memory_space=pl.ANY)] * count,
        scratch_shapes=[pltpu.VMEM(v.shape, v.dtype) for v in values] + [pltpu.SemaphoreType.DMA((2, count))],
        compiler_params=pltpu.CompilerParams(vmem_limit_bytes=60 * 1024 * 1024),
    )(*values)


def solution(mesh, sizes=(4, 8, 8, 2)):
    torus = Mesh(mesh.devices.reshape(sizes), ("x", "y", "z", "c"))
    row, col = ("x", "y"), ("z", "c")

    def body(activations, cotangents, weights, momentum, right_basis, next_inputs):
        shapes = dict(act=activations.shape, cot=cotangents.shape, nxt=next_inputs.shape)
        results = build(torus, shapes)(activations, cotangents, weights, momentum, right_basis, next_inputs)
        return placed(results)

    return jax.shard_map(
        body,
        mesh=torus,
        in_specs=(P(row, col), P(col, row), P(row, col), P(row, col), P(None, col), P(row, col)),
        out_specs=(P(row, col), P(row, col), P(None, col), P(col, row)),
        check_vma=False,
    )
```
